128 devices in a mesh: lat: 8 (over x, core), lon: 4 (over y), lev: 4 (over z).
Axes of the slice: x: 4, y: 4, z: 4, core: 2. Of those that a mesh axis runs over, the one named last changes fastest.
Arguments:
- initial_state: float32 [32, 384, 128, 128], P('lat', 'lon', 'lev'), may hold values from 0.5 to 2
- scaled_wind_north: float32 [32, 384, 128, 128], P('lat', 'lon', 'lev'), may hold values from -0.3 to 0.3
- scaled_wind_east: float32 [32, 384, 128, 128], P('lat', 'lon', 'lev'), may hold values from -0.3 to 0.3
- scaled_wind_upward: float32 [32, 384, 128, 128], P('lat', 'lon', 'lev'), may hold values from -0.3 to 0.3
Outputs:
- normalised_state: float32 [32, 384, 128, 128], P('lat', 'lon', 'lev')
- temperature_end: float32 [32, 384, 128, 128], P('lat', 'lon', 'lev')
The draws below stay inside these ranges and needn't reach their ends.
All inputs are finite; a program needn't handle non-finite values.
Results may differ from the reference program's by a relative error of at most 0.00002.
Values sent between devices are 32-bit elements; how exact they have to be, the bound alone decides.
No kernel may reach another device: no remote copies, remote signals or barrier semaphores. Data moves between devices by JAX's collectives and lax.ppermute only.
A program may use at most 128 MiB of HBM per device.

```python
import jax
import jax.numpy as jnp
from jax import lax

CELLS_NORTHWARD = 32
CELLS_EASTWARD = 384
CELLS_UPWARD = 128
MEMBER_TOTAL = 128
STEPS = 4


def block_scale(rng, extent, pieces, low, high):
    def one(position, blocks):
        steps = jax.random.uniform(jax.random.fold_in(jax.random.fold_in(rng, 6), position), (blocks,), jnp.float32, low / len(pieces), high / len(pieces))
        return jnp.repeat(jnp.exp(steps), extent[position] // blocks).reshape((-1,) + (1,) * (len(extent) - position - 1))

    gain = one(*pieces[0])
    for cut in pieces[1:]:
        gain = gain * one(*cut)
    return gain


def setup_inputs(seed: int = 0) -> dict:
    key_of = jax.random.split(jax.random.key(seed), 5)
    return {
        "initial_state": jnp.clip(0.5 + 1.5 * jax.random.uniform(key_of[0], (CELLS_NORTHWARD, CELLS_EASTWARD, CELLS_UPWARD, MEMBER_TOTAL), jnp.float32) ** block_scale(key_of[0], (CELLS_NORTHWARD, CELLS_EASTWARD, CELLS_UPWARD, MEMBER_TOTAL), ((0, 8), (1, 4), (2, 4)), -0.2, 0.2), 0.5, 2.0),
        "scaled_wind_north": jnp.clip(jax.random.uniform(key_of[1], (CELLS_NORTHWARD, CELLS_EASTWARD, CELLS_UPWARD, MEMBER_TOTAL), jnp.float32, -0.3, 0.3) * block_scale(key_of[1], (CELLS_NORTHWARD, CELLS_EASTWARD, CELLS_UPWARD, MEMBER_TOTAL), ((0, 8), (1, 4), (2, 4)), -0.4, 0.0), -0.3, 0.3),
        "scaled_wind_east": jnp.clip(jax.random.uniform(key_of[2], (CELLS_NORTHWARD, CELLS_EASTWARD, CELLS_UPWARD, MEMBER_TOTAL), jnp.float32, -0.3, 0.3) * block_scale(key_of[2], (CELLS_NORTHWARD, CELLS_EASTWARD, CELLS_UPWARD, MEMBER_TOTAL), ((0, 8), (1, 4), (2, 4)), -0.4, 0.0), -0.3, 0.3),
        "scaled_wind_upward": jnp.clip(jax.random.uniform(key_of[3], (CELLS_NORTHWARD, CELLS_EASTWARD, CELLS_UPWARD, MEMBER_TOTAL), jnp.float32, -0.3, 0.3) * block_scale(key_of[3], (CELLS_NORTHWARD, CELLS_EASTWARD, CELLS_UPWARD, MEMBER_TOTAL), ((0, 8), (1, 4), (2, 4)), -0.4, 0.0), -0.3, 0.3),
    }


def strip_edges(values, dims):
    for dim in dims:
        values = lax.slice_in_dim(values, 1, values.shape[dim] - 1, axis=dim)
    return values

def neighbour(values, dim, start, dims):
    others = [other for other in dims if other != dim]
    values = strip_edges(values, others)
    return lax.slice_in_dim(values, start, start + values.shape[dim] - 2, axis=dim)

def march_one_step(padded_state, scaled_wind_north, scaled_wind_east, scaled_wind_upward):
    middle = strip_edges(padded_state, (0, 1, 2))
    lower = [neighbour(padded_state, dim, 0, (0, 1, 2)) for dim in (0, 1, 2)]
    upper = [neighbour(padded_state, dim, 2, (0, 1, 2)) for dim in (0, 1, 2)]
    slopes = [above - below for above, below in zip(upper, lower)]
    smooth_rate = 0.05
    spread = lower[0] + upper[0] + lower[1] + upper[1] + lower[2] + upper[2] - 6.0 * middle
    return middle - scaled_wind_north * slopes[0] - scaled_wind_east * slopes[1] - scaled_wind_upward * slopes[2] + smooth_rate * spread

def reference(initial_state, scaled_wind_north, scaled_wind_east, scaled_wind_upward):
    for step in range(STEPS):
        initial_state = march_one_step(jnp.pad(initial_state, ((1, 1), (1, 1), (1, 1), (0, 0)), mode='constant'), scaled_wind_north, scaled_wind_east, scaled_wind_upward)
    vertical_mean = lax.optimization_barrier(jnp.mean(initial_state, axis=1, keepdims=True))
    symmetric_slope = initial_state - vertical_mean
    line_variance = lax.optimization_barrier(jnp.mean(symmetric_slope * symmetric_slope, axis=1, keepdims=True))
    normalised_state = symmetric_slope * lax.rsqrt(line_variance + 0.0001)
    return (normalised_state, initial_state)
```

```python
import functools

import jax
import jax.numpy as jnp
from jax import lax
from jax.experimental import pallas as pl
from jax.experimental.pallas import tpu as pltpu
from jax.sharding import PartitionSpec as P


STEPS = 4
RATE = 0.05
GRID = P("lat", "lon", "lev", None)


def roles(odd):
    first = 3 * odd
    turn = 1 - 2 * odd
    sign = jnp.where(odd == 0, 1.0, -1.0).astype(jnp.float32)
    return [first + turn * k for k in range(4)], sign


def either(flag, a, b):
    return jnp.where(flag, a, b)


def take_outer(place, source, outer, sem):
    rows, _ = roles(place[0])
    copy = pltpu.make_async_copy(source.at[rows[0]], outer, sem)
    copy.start()
    copy.wait()


def take_others(place, source, outer, *refs):
    others, ends, sems = refs[:3], refs[3:7], refs[7]
    rows, _ = roles(place[0])
    even_lev, even_lon = place[1] == 0, place[2] == 0
    copies = [
        pltpu.make_async_copy(source.at[rows[k + 1]], others[k], sems.at[k]) for k in range(3)
    ]
    for copy in copies:
        copy.start()
    for k in range(4):
        if k > 0:
            copies[k - 1].wait()
        row = outer if k == 0 else others[k - 1]
        send_ends(k, row, ends, even_lev, even_lon)


def send_ends(k, row, ends, even_lev, even_lon):
    length, levels, _ = row.shape

    def body(x, carry):
        low, high = row[x, 0:1], row[x, levels - 1 : levels]
        ends[0][k, pl.ds(x, 1)] = either(even_lev, high, low)
        ends[1][k, pl.ds(x, 1)] = either(even_lev, low, high)
        return carry

    lax.fori_loop(0, length, body, 0, unroll=4)
    low, high = row[0], row[length - 1]
    ends[2][k] = either(even_lon, high, low)
    ends[3][k] = either(even_lon, low, high)


def spread_step(last, place, *refs):
    state, refs = refs[:4], refs[4:]
    core_row, near_lev, far_lev, near_lon, far_lon, north, east, upward = refs[:8]
    new = refs[8:12]
    extra = refs[12:]
    rows, sign = roles(place[0])
    length, levels, members = new[0].shape
    even_lev, even_lon = place[1] == 0, place[2] == 0
    level = lax.broadcasted_iota(jnp.int32, (levels, members), 0)
    for k in range(4):
        row = rows[k]
        inward = core_row if k == 3 else state[k + 1]
        outward = None if k == 0 else state[k - 1]

        def cell(x, before, here, after):
            lower = either(even_lev, far_lev[k, pl.ds(x, 1)], near_lev[k, pl.ds(x, 1)])
            upper = either(even_lev, near_lev[k, pl.ds(x, 1)], far_lev[k, pl.ds(x, 1)])
            down = jnp.where(level == 0, lower, pltpu.roll(here, 1, 0))
            up = jnp.where(level == levels - 1, upper, pltpu.roll(here, levels - 1, 0))
            inner = inward[x]
            total = (before + after) + (down + up)
            if outward is None:
                total += inner
                slope = inner
            else:
                outer = outward[x]
                total += inner + outer
                slope = inner - outer
            value = (
                (1.0 - 6.0 * RATE) * here
                + RATE * total
                - (sign * north[row, x]) * slope
                - east[row, x] * (after - before)
                - upward[row, x] * (up - down)
            )
            new[k][x] = value
            if not last and k > 0:
                low, high = value[0:1], value[levels - 1 : levels]
                extra[0][k, pl.ds(x, 1)] = either(even_lev, high, low)
                extra[1][k, pl.ds(x, 1)] = either(even_lev, low, high)
            return value

        start = either(even_lon, far_lon[k], near_lon[k])
        stop = either(even_lon, near_lon[k], far_lon[k])

        def body(x, carry):
            before, here, total = carry
            after = state[k][x + 1]
            value = cell(x, before, here, after)
            return here, after, (total + value if last else total)

        zero = jnp.zeros((levels, members), jnp.float32)
        before, here, total = lax.fori_loop(
            0, length - 1, body, (start, state[k][0], zero), unroll=5
        )
        value = cell(length - 1, before, here, stop)
        if not last and k > 0:
            low, high = new[k][0], value
            extra[2][k] = either(even_lon, high, low)
            extra[3][k] = either(even_lon, low, high)
        if last and k > 0:
            line_statistics(new[k], total + value, extra[0], 2 * (k - 1))


def line_statistics(row, total, out, at):
    length = row.shape[0]
    mean = total * (1.0 / length)

    def body(x, carry):
        away = row[x] - mean
        return carry + away * away

    out[at] = mean
    out[at + 1] = lax.fori_loop(0, length, body, jnp.zeros_like(mean), unroll=4)


def finish_row(last, place, *refs):
    part, north, halo = refs[:3]
    rows, sign = roles(place[0])
    row = rows[0]
    length, levels, members = part.shape
    if last:
        out, stats = refs[3:]
    else:
        out, ends = refs[7], refs[8:]
        for old, end in zip(refs[3:7], ends):
            end[1:] = old[1:]
    even_lev, even_lon = place[1] == 0, place[2] == 0

    def body(x, total):
        value = part[x] + (RATE + sign * north[row, x]) * halo[x]
        out[x] = value
        if last:
            return total + value
        low, high = value[0:1], value[levels - 1 : levels]
        ends[0][0, pl.ds(x, 1)] = either(even_lev, high, low)
        ends[1][0, pl.ds(x, 1)] = either(even_lev, low, high)
        return total

    total = lax.fori_loop(0, length, body, jnp.zeros((levels, members), jnp.float32), unroll=4)
    if last:
        line_statistics(out, total, stats, 0)
    else:
        low, high = out[0], out[length - 1]
        ends[2][0] = either(even_lon, high, low)
        ends[3][0] = either(even_lon, low, high)


def normalise(count, place, *refs):
    state, stats = refs[:count], refs[count : count + 4]
    begin = count + 4 + (2 if count == 1 else 0)
    normal_out, end_out, work, sems = refs[begin:]
    rows, _ = roles(place[0])
    length = state[0].shape[0]
    offset = 1 if count > 1 else 0
    copies = []
    for k in range(count):
        copy = pltpu.make_async_copy(state[k], end_out.at[rows[k + offset]], sems.at[2 * k])
        copy.start()
        copies.append(copy)
    for k in range(count):
        means = [s[2 * k] for s in stats]
        mean = 0.25 * ((means[0] + means[1]) + (means[2] + means[3]))
        square = (stats[0][2 * k + 1] + stats[1][2 * k + 1]) + (
            stats[2][2 * k + 1] + stats[3][2 * k + 1]
        )
        for part in means:
            square += length * ((part - mean) * (part - mean))
        scale = lax.rsqrt(square * (1.0 / (4 * length)) + 0.0001)

        def body(x, carry):
            work[k, x] = (state[k][x] - mean) * scale
            return carry

        lax.fori_loop(0, length, body, 0, unroll=4)
        copy = pltpu.make_async_copy(work.at[k], normal_out.at[rows[k + offset]], sems.at[2 * k + 1])
        copy.start()
        copies.append(copy)
    for copy in copies:
        copy.wait()


def shards(initial_state, north, east, upward):
    rows_here, length, levels, members = initial_state.shape
    row_type = jax.ShapeDtypeStruct((length, levels, members), jnp.float32)
    lev_type = jax.ShapeDtypeStruct((rows_here, length, members), jnp.float32)
    lon_type = jax.ShapeDtypeStruct((rows_here, levels, members), jnp.float32)
    whole = jax.ShapeDtypeStruct(initial_state.shape, jnp.float32)
    vmem = pl.BlockSpec(memory_space=pltpu.VMEM)
    smem = pl.BlockSpec(memory_space=pltpu.SMEM)
    anywhere = pl.BlockSpec(memory_space=pl.ANY)
    place = jnp.stack([lax.rem(lax.axis_index(a), 2) for a in ("lat", "lev", "lon")])

    def call(kernel, args, outs, flops, aliases={}, in_specs=None, out_specs=None, scratch=()):
        return pl.pallas_call(
            kernel,
            out_shape=outs,
            in_specs=[smem] + (in_specs or [vmem] * len(args)),
            out_specs=out_specs or [vmem] * len(outs),
            scratch_shapes=list(scratch),
            input_output_aliases=aliases,
            compiler_params=pltpu.CompilerParams(vmem_limit_bytes=VMEM_LIMIT),
            cost_estimate=pl.CostEstimate(flops=flops, bytes_accessed=0, transcendentals=0),
        )(place, *args)

    lats, lons = lax.axis_size("lat"), lax.axis_size("lon")

    def pairs(count, start):
        out = []
        for i in range(start, count - 1, 2):
            out += [(i, i + 1), (i + 1, i)]
        return out

    def across(array):
        return lax.ppermute(array, "lat", pairs(lats, 1))

    def beside(array):
        return lax.ppermute(array, "lat", pairs(lats, 0))

    def swap(array, axis, start):
        return lax.ppermute(array, axis, pairs(lax.axis_size(axis), start))

    def ends_of(near_lev, far_lev, near_lon, far_lon):
        return [
            swap(near_lev, "lev", 0),
            swap(far_lev, "lev", 1),
            swap(near_lon, "lon", 0),
            swap(far_lon, "lon", 1),
        ]

    def from_others(array):
        return [lax.ppermute(array, "lon", [(i, i ^ d) for i in range(lons)]) for d in (1, 2, 3)]

    end_types = [lev_type, lev_type, lon_type, lon_type]
    source = pltpu.with_memory_space_constraint(initial_state, pltpu.HBM)
    winds = [pltpu.with_memory_space_constraint(w, pltpu.VMEM) for w in (north, east, upward)]
    for step in range(STEPS):
        last = step == STEPS - 1
        if step == 0:
            (outer,) = call(
                take_outer,
                [source],
                [row_type],
                10**6,
                in_specs=[anywhere],
                scratch=[pltpu.SemaphoreType.DMA],
            )
            halo = across(outer)
            *inner_rows, near, far, close, distant = call(
                take_others,
                [source, outer],
                [row_type] * 3 + end_types,
                10**9,
                in_specs=[anywhere, vmem],
                scratch=[pltpu.SemaphoreType.DMA((3,))],
            )
            core_row = beside(inner_rows[2])
            ends = ends_of(near, far, close, distant)
        else:
            outer, *sent = call(
                functools.partial(finish_row, False),
                [part, winds[0], halo, *extra],
                [row_type, *end_types],
                10**9,
            )
            halo = across(outer)
            ends = ends_of(*sent)
        part, *made = call(
            functools.partial(spread_step, last),
            [outer, *inner_rows, core_row, *ends, *winds],
            [row_type] * 4
            + ([jax.ShapeDtypeStruct((6, levels, members), jnp.float32)] if last else end_types),
            SPREAD_FLOPS,
        )
        inner_rows, extra = made[:3], made[3:]
        if not last:
            core_row = beside(inner_rows[2])
        else:
            stats = extra[0]
            shared = from_others(stats)
            results = call(
                functools.partial(normalise, 3),
                [*inner_rows, stats, *shared],
                [whole, whole],
                SPREAD_FLOPS,
                out_specs=[anywhere, anywhere],
                scratch=[
                    pltpu.VMEM((3, length, levels, members), jnp.float32),
                    pltpu.SemaphoreType.DMA((6,)),
                ],
            )
    outer, stats = call(
        functools.partial(finish_row, True),
        [part, winds[0], halo],
        [row_type, jax.ShapeDtypeStruct((2, levels, members), jnp.float32)],
        10**9,
    )
    results = call(
        functools.partial(normalise, 1),
        [outer, stats, *from_others(stats), *results],
        [whole, whole],
        10**9,
        aliases={6: 0, 7: 1},
        in_specs=[vmem] * 5 + [anywhere] * 2,
        out_specs=[anywhere, anywhere],
        scratch=[
            pltpu.VMEM((1, length, levels, members), jnp.float32),
            pltpu.SemaphoreType.DMA((2,)),
        ],
    )
    return tuple(results)


VMEM_LIMIT = 12 * 2**20
SPREAD_FLOPS = 2 * 10**10


def solution(mesh):
    return jax.shard_map(
        shards, mesh=mesh, in_specs=(GRID,) * 4, out_specs=(GRID, GRID), check_vma=False
    )
```

```python
import functools

import jax
import jax.numpy as jnp
from jax import lax
from jax.experimental import pallas as pl
from jax.experimental.pallas import tpu as pltpu
from jax.sharding import PartitionSpec as P


STEPS = 4
TILE = 8
UNROLL = 19
PIECES = 2
RATE = 0.05
GRID = P("lat", "lon", "lev", None)


def here():
    return [lax.rem(lax.axis_index(axis), 2) for axis in ("lat", "lev", "lon")]


def roles(odd):
    first = 3 * odd
    turn = 1 - 2 * odd
    sign = jnp.where(odd == 0, 1.0, -1.0).astype(jnp.float32)
    return [first + turn * k for k in range(4)], sign


def either(flag, a, b):
    return jnp.where(flag, a, b)


def take_outer(source, *refs):
    place = here()
    pieces, sems = refs[:PIECES], refs[PIECES]
    rows, _ = roles(place[0])
    size = pieces[0].shape[0]
    copies = [
        pltpu.make_async_copy(source.at[rows[0], pl.ds(size * p, size)], pieces[p], sems.at[p])
        for p in range(PIECES)
    ]
    for copy in copies:
        copy.start()
    for copy in copies:
        copy.wait()


def take_all(source, *refs):
    place = here()
    taken, ends, sems = refs[:4], refs[4:8], refs[8]
    rows, _ = roles(place[0])
    even_lev, even_lon = place[1] == 0, place[2] == 0
    copies = [pltpu.make_async_copy(source.at[rows[k]], taken[k], sems.at[k]) for k in range(4)]
    for copy in copies:
        copy.start()
    for k in range(4):
        copies[k].wait()
        send_ends(k, taken[k], ends, even_lev, even_lon)


def send_ends(k, row, ends, even_lev, even_lon):
    length, levels, _ = row.shape

    def body(x, carry):
        low, high = row[x, 0:1], row[x, levels - 1 : levels]
        ends[0][k, pl.ds(x, 1)] = either(even_lev, high, low)
        ends[1][k, pl.ds(x, 1)] = either(even_lev, low, high)
        return carry

    lax.fori_loop(0, length, body, 0, unroll=4)
    low, high = row[0], row[length - 1]
    ends[2][k] = either(even_lon, high, low)
    ends[3][k] = either(even_lon, low, high)


def spread_step(last, *refs):
    place = here()
    for odd in (0, 1):
        pl.when(place[0] == odd)(functools.partial(spread_rows, last, odd, place, *refs))


def spread_rows(last, odd, place, *refs):
    state, refs = refs[:4], refs[4:]
    core_row, near_lev, far_lev, near_lon, far_lon, north, east, upward = refs[:8]
    new = refs[8:12]
    extra = refs[12:]
    rows, _ = roles(odd)
    length, levels, members = new[0].shape
    even_lev, even_lon = place[1] == 0, place[2] == 0
    parts = levels // TILE
    spot = lax.broadcasted_iota(jnp.int32, (TILE, members), 0)
    at_low, at_high = spot == 0, spot == TILE - 1
    for k in range(4):
        row = rows[k]
        inward = core_row if k == 3 else state[k + 1]
        outward = None if k == 0 else state[k - 1]

        def cell(x, before, here, after):
            near, far = near_lev[k, pl.ds(x, 1)], far_lev[k, pl.ds(x, 1)]
            lower, upper = either(even_lev, far, near), either(even_lev, near, far)
            tiles = [here[TILE * j : TILE * (j + 1)] for j in range(parts)]
            from_below = [lower] + [pltpu.roll(t, 1, 0) for t in tiles]
            from_above = [pltpu.roll(t, TILE - 1, 0) for t in tiles] + [upper]
            values = []
            for j in range(parts):
                cut = slice(TILE * j, TILE * (j + 1))
                down = jnp.where(at_low, from_below[j], from_below[j + 1])
                up = jnp.where(at_high, from_above[j + 1], from_above[j])
                inner = inward[x, cut]
                total = (before[cut] + after[cut]) + (down + up)
                if outward is None:
                    total += inner
                    slope = inner
                else:
                    outer = outward[x, cut]
                    total += inner + outer
                    slope = outer - inner if odd else inner - outer
                drift = north[row, x, cut] * slope
                value = (1.0 - 6.0 * RATE) * tiles[j] + RATE * total
                value = value + drift if odd and outward is None else value - drift
                value = (
                    value
                    - east[row, x, cut] * (after[cut] - before[cut])
                    - upward[row, x, cut] * (up - down)
                )
                new[k][x, cut] = value
                values.append(value)
            if not last and k > 0:
                low, high = values[0][0:1], values[-1][TILE - 1 : TILE]
                extra[0][k, pl.ds(x, 1)] = either(even_lev, high, low)
                extra[1][k, pl.ds(x, 1)] = either(even_lev, low, high)
            return jnp.concatenate(values, axis=0)

        start = either(even_lon, far_lon[k], near_lon[k])
        stop = either(even_lon, near_lon[k], far_lon[k])

        def body(x, carry):
            before, here, total = carry
            after = state[k][x + 1]
            value = cell(x, before, here, after)
            return here, after, (total + value if last else total)

        zero = jnp.zeros((levels, members), jnp.float32)
        before, here, total = lax.fori_loop(
            0, length - 1, body, (start, state[k][0], zero), unroll=UNROLL
        )
        value = cell(length - 1, before, here, stop)
        if not last and k > 0:
            low, high = new[k][0], value
            extra[2][k] = either(even_lon, high, low)
            extra[3][k] = either(even_lon, low, high)
        if last and k > 0:
            line_statistics(new[k], total + value, extra[0], 2 * (k - 1))


def line_statistics(row, total, out, at):
    length = row.shape[0]
    mean = total * (1.0 / length)

    def body(x, carry):
        away = row[x] - mean
        return carry + away * away

    out[at] = mean
    out[at + 1] = lax.fori_loop(0, length, body, jnp.zeros_like(mean), unroll=4)


def add_halo(piece, place, part, north, halo, out, inner=None):
    rows, sign = roles(place[0])
    size, levels, members = halo.shape

    def body(x, total):
        at = size * piece + x
        value = part[at] + (RATE + sign * north[rows[0], at]) * halo[x]
        out[x] = value
        if inner is not None:
            inner(at, value)
        return total + value

    zero = jnp.zeros((levels, members), jnp.float32)
    return lax.fori_loop(0, size, body, zero, unroll=4)


def start_row(part, north, halo, out):
    add_halo(0, here(), part, north, halo, out)


def finish_row(last, *refs):
    place = here()
    part, north, halo, done = refs[:4]
    rest = refs[4:]
    size, levels, members = halo.shape
    if last:
        row, stats = rest
    else:
        old, piece, row, ends = rest[:4], rest[4], rest[5], rest[6:]
        for a, b in zip(old, ends):
            b[1:] = a[1:]
    even_lev, even_lon = place[1] == 0, place[2] == 0

    def send(at, value):
        if not last:
            low, high = value[0:1], value[levels - 1 : levels]
            ends[0][0, pl.ds(at, 1)] = either(even_lev, high, low)
            ends[1][0, pl.ds(at, 1)] = either(even_lev, low, high)

    def keep(x, total):
        value = done[x]
        row[x] = value
        send(x, value)
        return total + value

    def both(at, value):
        if not last:
            row[at] = value
        send(at, value)

    zero = jnp.zeros((levels, members), jnp.float32)
    total = lax.fori_loop(0, size, keep, zero, unroll=4)
    if last:
        total += add_halo(1, place, part, north, halo, row.at[pl.ds(size, size)])
        line_statistics(row, total, stats, 0)
    else:
        add_halo(1, place, part, north, halo, piece, both)
        low, high = row[0], row[2 * size - 1]
        ends[2][0] = either(even_lon, high, low)
        ends[3][0] = either(even_lon, low, high)


def normalise(count, *refs):
    state, stats = refs[:count], refs[count : count + 4]
    out, end, work, sems = refs[-4:]
    rows, _ = roles(here()[0])
    offset = 0 if count == 1 else 1
    length = state[0].shape[0]
    copies = [
        pltpu.make_async_copy(state[k], end.at[rows[k + offset]], sems.at[k]) for k in range(count)
    ]
    for copy in copies:
        copy.start()
    for k in range(count):
        means = [s[2 * k] for s in stats]
        mean = 0.25 * ((means[0] + means[1]) + (means[2] + means[3]))
        square = (stats[0][2 * k + 1] + stats[1][2 * k + 1]) + (
            stats[2][2 * k + 1] + stats[3][2 * k + 1]
        )
        for part in means:
            square += length * ((part - mean) * (part - mean))
        scale = lax.rsqrt(square * (1.0 / (4 * length)) + 0.0001)

        def body(x, carry):
            work[k, x] = (state[k][x] - mean) * scale
            return carry

        lax.fori_loop(0, length, body, 0, unroll=4)
        copy = pltpu.make_async_copy(work.at[k], out.at[rows[k + offset]], sems.at[count + k])
        copy.start()
        copies.append(copy)
    for copy in copies:
        copy.wait()


def shards(initial_state, north, east, upward):
    rows_here, length, levels, members = initial_state.shape
    row_type = jax.ShapeDtypeStruct((length, levels, members), jnp.float32)
    piece_type = jax.ShapeDtypeStruct((length // PIECES, levels, members), jnp.float32)
    lev_type = jax.ShapeDtypeStruct((rows_here, length, members), jnp.float32)
    lon_type = jax.ShapeDtypeStruct((rows_here, levels, members), jnp.float32)
    whole = jax.ShapeDtypeStruct(initial_state.shape, jnp.float32)
    vmem = pl.BlockSpec(memory_space=pltpu.VMEM)
    anywhere = pl.BlockSpec(memory_space=pl.ANY)

    def call(kernel, args, outs, flops, aliases={}, in_specs=None, out_specs=None, scratch=(), room=2**20):
        return pl.pallas_call(
            kernel,
            out_shape=outs,
            in_specs=in_specs or [vmem] * len(args),
            out_specs=out_specs or [vmem] * len(outs),
            scratch_shapes=list(scratch),
            input_output_aliases=aliases,
            compiler_params=pltpu.CompilerParams(vmem_limit_bytes=room),
            cost_estimate=pl.CostEstimate(flops=flops, bytes_accessed=0, transcendentals=0),
        )(*args)

    lats, lons = lax.axis_size("lat"), lax.axis_size("lon")

    def pairs(count, start):
        out = []
        for i in range(start, count - 1, 2):
            out += [(i, i + 1), (i + 1, i)]
        return out

    def across(array):
        return lax.ppermute(array, "lat", pairs(lats, 1))

    def beside(array):
        return lax.ppermute(array, "lat", pairs(lats, 0))

    def swap(array, axis, start):
        return lax.ppermute(array, axis, pairs(lax.axis_size(axis), start))

    def ends_of(near_lev, far_lev, near_lon, far_lon):
        return [
            swap(near_lev, "lev", 0),
            swap(far_lev, "lev", 1),
            swap(near_lon, "lon", 0),
            swap(far_lon, "lon", 1),
        ]

    def from_others(array):
        made = []
        for d in (1, 2, 3):
            made.append(lax.ppermute(array, "lon", [(i, i ^ d) for i in range(lons)]))
        return made

    stats_type = jax.ShapeDtypeStruct((2 * rows_here - 2, levels, members), jnp.float32)
    end_types = [lev_type, lev_type, lon_type, lon_type]
    source = pltpu.with_memory_space_constraint(initial_state, pltpu.HBM)
    winds = [pltpu.with_memory_space_constraint(w, pltpu.VMEM) for w in (north, east, upward)]
    for step in range(STEPS):
        last = step == STEPS - 1
        if step == 0:
            pieces = call(
                take_outer,
                [source],
                [piece_type] * PIECES,
                10**6,
                in_specs=[anywhere],
                scratch=[pltpu.SemaphoreType.DMA((PIECES,))],
            )
            halos = [across(piece) for piece in pieces]
            outer, *inner_rows, near, far, close, distant = call(
                take_all,
                [source],
                [row_type] * 4 + end_types,
                10**9,
                in_specs=[anywhere],
                scratch=[pltpu.SemaphoreType.DMA((4,))],
            )
            core_row = beside(inner_rows[2])
            ends = ends_of(near, far, close, distant)
        else:
            (begun,) = call(
                start_row, [part, winds[0], halos[0]], [piece_type], 10**9
            )
            first_halo = across(begun)
            ended, outer, *sent = call(
                functools.partial(finish_row, False),
                [part, winds[0], halos[1], begun, *extra],
                [piece_type, row_type, *end_types],
                10**9,
            )
            halos = [first_halo, across(ended)]
            ends = ends_of(*sent)
        part, *made = call(
            functools.partial(spread_step, last),
            [outer, *inner_rows, core_row, *ends, *winds],
            [row_type] * 4 + ([stats_type] if last else end_types),
            SPREAD_FLOPS,
        )
        inner_rows, extra = made[:3], made[3:]
        if not last:
            core_row = beside(inner_rows[2])

    def normalised(rows_of, stats, others, *results):
        count = len(rows_of)
        return call(
            functools.partial(normalise, count),
            [*rows_of, stats, *others, *results],
            [whole, whole],
            10**9,
            aliases={count + 4 + i: i for i in range(len(results))},
            in_specs=[vmem] * (count + 4) + [anywhere] * len(results),
            out_specs=[anywhere, anywhere],
            scratch=[
                pltpu.VMEM((count, length, levels, members), jnp.float32),
                pltpu.SemaphoreType.DMA((2 * count,)),
            ],
            room=8 * 2**20,
        )

    (begun,) = call(start_row, [part, winds[0], halos[0]], [piece_type], 10**9)
    early = from_others(extra[0])
    outer, stats = call(
        functools.partial(finish_row, True),
        [part, winds[0], halos[1], begun],
        [row_type, jax.ShapeDtypeStruct((2, levels, members), jnp.float32)],
        10**9,
    )
    late = from_others(stats)
    results = normalised(inner_rows, extra[0], early)
    return tuple(normalised([outer], stats, late, *results))


SPREAD_FLOPS = 2 * 10**10


def solution(mesh):
    return jax.shard_map(
        shards, mesh=mesh, in_specs=(GRID,) * 4, out_specs=(GRID, GRID), check_vma=False
    )
```

```python
import functools

import jax
import jax.numpy as jnp
from jax import lax
from jax.experimental import pallas as pl
from jax.experimental.pallas import tpu as pltpu
from jax.sharding import PartitionSpec as P


STEPS = 4
TILE = 8
UNROLL = 19
PIECES = 2
FIRST = 64
RATE = 0.05
GRID = P("lat", "lon", "lev", None)


def here():
    return [lax.rem(lax.axis_index(axis), 2) for axis in ("lat", "lev", "lon")]


def roles(odd):
    first = 3 * odd
    turn = 1 - 2 * odd
    sign = jnp.where(odd == 0, 1.0, -1.0).astype(jnp.float32)
    return [first + turn * k for k in range(4)], sign


def either(flag, a, b):
    return jnp.where(flag, a, b)


def take_outer(source, *refs):
    place = here()
    pieces, sems = refs[:PIECES], refs[PIECES]
    rows, _ = roles(place[0])
    copies, at = [], 0
    for p, piece in enumerate(pieces):
        size = piece.shape[0]
        copies.append(
            pltpu.make_async_copy(source.at[rows[0], pl.ds(at, size)], piece, sems.at[p])
        )
        at += size
    for copy in copies:
        copy.start()
    for copy in copies:
        copy.wait()


def take_all(source, *refs):
    place = here()
    taken, ends, sems = refs[:4], refs[4:8], refs[8]
    rows, _ = roles(place[0])
    even_lev, even_lon = place[1] == 0, place[2] == 0
    copies = [pltpu.make_async_copy(source.at[rows[k]], taken[k], sems.at[k]) for k in range(4)]
    for copy in copies:
        copy.start()
    for k in range(4):
        copies[k].wait()
        send_ends(k, taken[k], ends, even_lev, even_lon)


def send_ends(k, row, ends, even_lev, even_lon):
    length, levels, _ = row.shape

    def body(x, carry):
        low, high = row[x, 0:1], row[x, levels - 1 : levels]
        ends[0][k, pl.ds(x, 1)] = either(even_lev, high, low)
        ends[1][k, pl.ds(x, 1)] = either(even_lev, low, high)
        return carry

    lax.fori_loop(0, length, body, 0, unroll=4)
    low, high = row[0], row[length - 1]
    ends[2][k] = either(even_lon, high, low)
    ends[3][k] = either(even_lon, low, high)


def spread_step(first, last, *refs):
    place = here()
    for odd in (0, 1):
        pl.when(place[0] == odd)(functools.partial(spread_rows, first, last, odd, place, *refs))


def spread_rows(first, last, odd, place, *refs):
    state, refs = refs[:4], refs[4:]
    core_row, near_lev, far_lev, near_lon, far_lon, north, east, upward = refs[:8]
    new = refs[8:12]
    extra = refs[12:]
    rows, _ = roles(odd)
    if first:
        stored, (upward, sems) = upward, extra[-2:]
        loads = [
            pltpu.make_async_copy(stored.at[row], upward.at[row], sems.at[row]) for row in rows
        ]
        for load in loads:
            load.start()
    length, levels, members = new[0].shape
    even_lev, even_lon = place[1] == 0, place[2] == 0
    parts = levels // TILE
    spot = lax.broadcasted_iota(jnp.int32, (TILE, members), 0)
    at_low, at_high = spot == 0, spot == TILE - 1
    for k in range(4):
        row = rows[k]
        if first:
            loads[k].wait()
        inward = core_row if k == 3 else state[k + 1]
        outward = None if k == 0 else state[k - 1]

        def cell(x, before, here, after):
            near, far = near_lev[k, pl.ds(x, 1)], far_lev[k, pl.ds(x, 1)]
            lower, upper = either(even_lev, far, near), either(even_lev, near, far)
            tiles = [here[TILE * j : TILE * (j + 1)] for j in range(parts)]
            from_below = [lower] + [pltpu.roll(t, 1, 0) for t in tiles]
            from_above = [pltpu.roll(t, TILE - 1, 0) for t in tiles] + [upper]
            values = []
            for j in range(parts):
                cut = slice(TILE * j, TILE * (j + 1))
                down = jnp.where(at_low, from_below[j], from_below[j + 1])
                up = jnp.where(at_high, from_above[j + 1], from_above[j])
                inner = inward[x, cut]
                total = (before[cut] + after[cut]) + (down + up)
                if outward is None:
                    total += inner
                    slope = inner
                else:
                    outer = outward[x, cut]
                    total += inner + outer
                    slope = outer - inner if odd else inner - outer
                drift = north[row, x, cut] * slope
                value = (1.0 - 6.0 * RATE) * tiles[j] + RATE * total
                value = value + drift if odd and outward is None else value - drift
                value = (
                    value
                    - east[row, x, cut] * (after[cut] - before[cut])
                    - upward[row, x, cut] * (up - down)
                )
                new[k][x, cut] = value
                values.append(value)
            if not last and k > 0:
                low, high = values[0][0:1], values[-1][TILE - 1 : TILE]
                extra[0][k, pl.ds(x, 1)] = either(even_lev, high, low)
                extra[1][k, pl.ds(x, 1)] = either(even_lev, low, high)
            return jnp.concatenate(values, axis=0)

        start = either(even_lon, far_lon[k], near_lon[k])
        stop = either(even_lon, near_lon[k], far_lon[k])

        def body(x, carry):
            before, here, total = carry
            after = state[k][x + 1]
            value = cell(x, before, here, after)
            return here, after, (total + value if last else total)

        zero = jnp.zeros((levels, members), jnp.float32)
        before, here, total = lax.fori_loop(
            0, length - 1, body, (start, state[k][0], zero), unroll=UNROLL
        )
        value = cell(length - 1, before, here, stop)
        if not last and k > 0:
            low, high = new[k][0], value
            extra[2][k] = either(even_lon, high, low)
            extra[3][k] = either(even_lon, low, high)
        if last and k > 0:
            line_statistics(new[k], total + value, extra[0], 2 * (k - 1))


def line_statistics(row, total, out, at):
    length = row.shape[0]
    mean = total * (1.0 / length)

    def body(x, carry):
        away = row[x] - mean
        return carry + away * away

    out[at] = mean
    out[at + 1] = lax.fori_loop(0, length, body, jnp.zeros_like(mean), unroll=4)


def add_halo(offset, place, part, north, halo, out, inner=None):
    rows, sign = roles(place[0])
    size, levels, members = halo.shape

    def body(x, total):
        at = offset + x
        value = part[at] + (RATE + sign * north[rows[0], at]) * halo[x]
        out[x] = value
        if inner is not None:
            inner(at, value)
        return total + value

    zero = jnp.zeros((levels, members), jnp.float32)
    return lax.fori_loop(0, size, body, zero, unroll=4)


def start_row(part, north, halo, out):
    add_halo(0, here(), part, north, halo, out)


def finish_row(last, *refs):
    place = here()
    part, north, halo, done = refs[:4]
    rest = refs[4:]
    size, (levels, members) = done.shape[0], halo.shape[1:]
    if last:
        row, stats = rest
    else:
        old, piece, row, ends = rest[:4], rest[4], rest[5], rest[6:]
        for a, b in zip(old, ends):
            b[1:] = a[1:]
    even_lev, even_lon = place[1] == 0, place[2] == 0

    def send(at, value):
        if not last:
            low, high = value[0:1], value[levels - 1 : levels]
            ends[0][0, pl.ds(at, 1)] = either(even_lev, high, low)
            ends[1][0, pl.ds(at, 1)] = either(even_lev, low, high)

    def keep(x, total):
        value = done[x]
        row[x] = value
        send(x, value)
        return total + value

    def both(at, value):
        if not last:
            row[at] = value
        send(at, value)

    zero = jnp.zeros((levels, members), jnp.float32)
    total = lax.fori_loop(0, size, keep, zero, unroll=4)
    if last:
        total += add_halo(size, place, part, north, halo, row.at[pl.ds(size, halo.shape[0])])
        line_statistics(row, total, stats, 0)
    else:
        add_halo(size, place, part, north, halo, piece, both)
        low, high = row[0], row[row.shape[0] - 1]
        ends[2][0] = either(even_lon, high, low)
        ends[3][0] = either(even_lon, low, high)


def normalise(count, *refs):
    state, stats = refs[:count], refs[count : count + 4]
    out, end, work, sems = refs[-4:]
    rows, _ = roles(here()[0])
    offset = 0 if count == 1 else 1
    length = state[0].shape[0]
    copies = [
        pltpu.make_async_copy(state[k], end.at[rows[k + offset]], sems.at[k]) for k in range(count)
    ]
    for copy in copies:
        copy.start()
    for k in range(count):
        means = [s[2 * k] for s in stats]
        mean = 0.25 * ((means[0] + means[1]) + (means[2] + means[3]))
        square = (stats[0][2 * k + 1] + stats[1][2 * k + 1]) + (
            stats[2][2 * k + 1] + stats[3][2 * k + 1]
        )
        for part in means:
            square += length * ((part - mean) * (part - mean))
        scale = lax.rsqrt(square * (1.0 / (4 * length)) + 0.0001)

        def body(x, carry):
            work[k, x] = (state[k][x] - mean) * scale
            return carry

        lax.fori_loop(0, length, body, 0, unroll=4)
        copy = pltpu.make_async_copy(work.at[k], out.at[rows[k + offset]], sems.at[count + k])
        copy.start()
        copies.append(copy)
    for copy in copies:
        copy.wait()


def placed(array, space):
    return pltpu.with_memory_space_constraint(array, space)


def shards(initial_state, north, east, upward):
    rows_here, length, levels, members = initial_state.shape
    row_type = jax.ShapeDtypeStruct((length, levels, members), jnp.float32)
    sizes = (length * FIRST // 96, length - length * FIRST // 96)
    piece_types = [jax.ShapeDtypeStruct((n, levels, members), jnp.float32) for n in sizes]
    lev_type = jax.ShapeDtypeStruct((rows_here, length, members), jnp.float32)
    lon_type = jax.ShapeDtypeStruct((rows_here, levels, members), jnp.float32)
    whole = jax.ShapeDtypeStruct(initial_state.shape, jnp.float32)
    vmem = pl.BlockSpec(memory_space=pltpu.VMEM)
    anywhere = pl.BlockSpec(memory_space=pl.ANY)

    def call(kernel, args, outs, flops, aliases={}, in_specs=None, out_specs=None, scratch=(), room=2**20):
        return pl.pallas_call(
            kernel,
            out_shape=outs,
            in_specs=in_specs or [vmem] * len(args),
            out_specs=out_specs or [vmem] * len(outs),
            scratch_shapes=list(scratch),
            input_output_aliases=aliases,
            compiler_params=pltpu.CompilerParams(vmem_limit_bytes=room),
            cost_estimate=pl.CostEstimate(flops=flops, bytes_accessed=0, transcendentals=0),
        )(*args)

    lats, lons = lax.axis_size("lat"), lax.axis_size("lon")

    def pairs(count, start):
        out = []
        for i in range(start, count - 1, 2):
            out += [(i, i + 1), (i + 1, i)]
        return out

    def across(array):
        return lax.ppermute(array, "lat", pairs(lats, 1))

    def beside(array):
        return lax.ppermute(array, "lat", pairs(lats, 0))

    def swap(array, axis, start):
        return lax.ppermute(array, axis, pairs(lax.axis_size(axis), start))

    def ends_of(near_lev, far_lev, near_lon, far_lon):
        return [
            swap(near_lev, "lev", 0),
            swap(far_lev, "lev", 1),
            swap(near_lon, "lon", 0),
            swap(far_lon, "lon", 1),
        ]

    def from_others(array):
        made = []
        for d in (1, 2, 3):
            made.append(lax.ppermute(array, "lon", [(i, i ^ d) for i in range(lons)]))
        return made

    stats_type = jax.ShapeDtypeStruct((2 * rows_here - 2, levels, members), jnp.float32)
    end_types = [lev_type, lev_type, lon_type, lon_type]
    source = placed(initial_state, pltpu.HBM)
    winds = [placed(north, pltpu.VMEM), placed(east, pltpu.VMEM), placed(upward, pltpu.HBM)]
    for step in range(STEPS):
        last = step == STEPS - 1
        if step == 0:
            pieces = call(
                take_outer,
                [source],
                piece_types,
                10**6,
                in_specs=[anywhere],
                scratch=[pltpu.SemaphoreType.DMA((PIECES,))],
            )
            halos = [across(piece) for piece in pieces]
            outer, *inner_rows, near, far, close, distant = call(
                take_all,
                [source],
                [row_type] * 4 + end_types,
                10**9,
                in_specs=[anywhere],
                scratch=[pltpu.SemaphoreType.DMA((4,))],
            )
            core_row = beside(inner_rows[2])
            ends = ends_of(near, far, close, distant)
        else:
            (begun,) = call(
                start_row, [part, winds[0], halos[0]], piece_types[:1], 10**9
            )
            first_halo = across(begun)
            ended, outer, *sent = call(
                functools.partial(finish_row, False),
                [part, winds[0], halos[1], begun, *extra],
                [piece_types[1], row_type, *end_types],
                10**9,
            )
            halos = [first_halo, across(ended)]
            ends = ends_of(*sent)
        part, *made = call(
            functools.partial(spread_step, step == 0, last),
            [outer, *inner_rows, core_row, *ends, *winds],
            [row_type] * 4
            + ([stats_type] if last else end_types)
            + ([whole] if step == 0 else []),
            SPREAD_FLOPS,
            in_specs=[vmem] * 11 + [anywhere if step == 0 else vmem],
            scratch=[pltpu.SemaphoreType.DMA((4,))] if step == 0 else [],
        )
        if step == 0:
            winds[2] = placed(made.pop(), pltpu.VMEM)
        inner_rows, extra = made[:3], made[3:]
        if not last:
            core_row = beside(inner_rows[2])

    def normalised(rows_of, stats, others, *results):
        count = len(rows_of)
        return call(
            functools.partial(normalise, count),
            [*rows_of, stats, *others, *results],
            [whole, whole],
            10**9,
            aliases={count + 4 + i: i for i in range(len(results))},
            in_specs=[vmem] * (count + 4) + [anywhere] * len(results),
            out_specs=[anywhere, anywhere],
            scratch=[
                pltpu.VMEM((count, length, levels, members), jnp.float32),
                pltpu.SemaphoreType.DMA((2 * count,)),
            ],
            room=8 * 2**20,
        )

    (begun,) = call(start_row, [part, winds[0], halos[0]], piece_types[:1], 10**9)
    early = from_others(extra[0])
    outer, stats = call(
        functools.partial(finish_row, True),
        [part, winds[0], halos[1], begun],
        [row_type, jax.ShapeDtypeStruct((2, levels, members), jnp.float32)],
        10**9,
    )
    late = from_others(stats)
    results = normalised(inner_rows, extra[0], early)
    return tuple(normalised([outer], stats, late, *results))


SPREAD_FLOPS = 2 * 10**10


def solution(mesh):
    return jax.shard_map(
        shards, mesh=mesh, in_specs=(GRID,) * 4, out_specs=(GRID, GRID), check_vma=False
    )
```

```python
import functools

import jax
import jax.numpy as jnp
from jax import lax
from jax.experimental import pallas as pl
from jax.experimental.pallas import tpu as pltpu
from jax.sharding import PartitionSpec as P


STEPS = 4
TILE = 8
UNROLL = 19
PIECES = 2
FIRST = 72
RATE = 0.05
GRID = P("lat", "lon", "lev", None)


def here():
    return [lax.rem(lax.axis_index(axis), 2) for axis in ("lat", "lev", "lon")]


def roles(odd):
    first = 3 * odd
    turn = 1 - 2 * odd
    sign = jnp.where(odd == 0, 1.0, -1.0).astype(jnp.float32)
    return [first + turn * k for k in range(4)], sign


def either(flag, a, b):
    return jnp.where(flag, a, b)


def take_outer(source, *refs):
    place = here()
    pieces, sems = refs[:PIECES], refs[PIECES]
    rows, _ = roles(place[0])
    copies, at = [], 0
    for p, piece in enumerate(pieces):
        size = piece.shape[0]
        copies.append(
            pltpu.make_async_copy(source.at[rows[0], pl.ds(at, size)], piece, sems.at[p])
        )
        at += size
    for copy in copies:
        copy.start()
    for copy in copies:
        copy.wait()


def take_all(source, *refs):
    place = here()
    taken, ends, sems = refs[:4], refs[4:8], refs[8]
    rows, _ = roles(place[0])
    even_lev, even_lon = place[1] == 0, place[2] == 0
    copies = [pltpu.make_async_copy(source.at[rows[k]], taken[k], sems.at[k]) for k in range(4)]
    for copy in copies:
        copy.start()
    for k in range(4):
        copies[k].wait()
        send_ends(k, taken[k], ends, even_lev, even_lon)


def send_ends(k, row, ends, even_lev, even_lon):
    length, levels, _ = row.shape

    def body(x, carry):
        low, high = row[x, 0:1], row[x, levels - 1 : levels]
        ends[0][k, pl.ds(x, 1)] = either(even_lev, high, low)
        ends[1][k, pl.ds(x, 1)] = either(even_lev, low, high)
        return carry

    lax.fori_loop(0, length, body, 0, unroll=4)
    low, high = row[0], row[length - 1]
    ends[2][k] = either(even_lon, high, low)
    ends[3][k] = either(even_lon, low, high)


def spread_step(first, last, *refs):
    place = here()
    for odd in (0, 1):
        pl.when(place[0] == odd)(functools.partial(spread_rows, first, last, odd, place, *refs))


def spread_rows(first, last, odd, place, *refs):
    state, refs = refs[:4], refs[4:]
    core_row, near_lev, far_lev, near_lon, far_lon, north, east, upward = refs[:8]
    new = refs[8:12]
    extra = refs[12:]
    rows, _ = roles(odd)
    if first:
        stored, (upward, sems) = upward, extra[-2:]
        loads = [
            pltpu.make_async_copy(stored.at[row], upward.at[row], sems.at[row]) for row in rows
        ]
        for load in loads:
            load.start()
    if last:
        end, sems = extra[1:]
        writes = [
            pltpu.make_async_copy(new[k], end.at[rows[k]], sems.at[k - 1]) for k in (1, 2, 3)
        ]
    length, levels, members = new[0].shape
    even_lev, even_lon = place[1] == 0, place[2] == 0
    parts = levels // TILE
    spot = lax.broadcasted_iota(jnp.int32, (TILE, members), 0)
    at_low, at_high = spot == 0, spot == TILE - 1
    for k in (1, 2, 3, 0) if last else range(4):
        row = rows[k]
        if first:
            loads[k].wait()
        inward = core_row if k == 3 else state[k + 1]
        outward = None if k == 0 else state[k - 1]

        def cell(x, before, here, after):
            near, far = near_lev[k, pl.ds(x, 1)], far_lev[k, pl.ds(x, 1)]
            lower, upper = either(even_lev, far, near), either(even_lev, near, far)
            tiles = [here[TILE * j : TILE * (j + 1)] for j in range(parts)]
            from_below = [lower] + [pltpu.roll(t, 1, 0) for t in tiles]
            from_above = [pltpu.roll(t, TILE - 1, 0) for t in tiles] + [upper]
            values = []
            for j in range(parts):
                cut = slice(TILE * j, TILE * (j + 1))
                down = jnp.where(at_low, from_below[j], from_below[j + 1])
                up = jnp.where(at_high, from_above[j + 1], from_above[j])
                inner = inward[x, cut]
                total = (before[cut] + after[cut]) + (down + up)
                if outward is None:
                    total += inner
                    slope = inner
                else:
                    outer = outward[x, cut]
                    total += inner + outer
                    slope = outer - inner if odd else inner - outer
                drift = north[row, x, cut] * slope
                value = (1.0 - 6.0 * RATE) * tiles[j] + RATE * total
                value = value + drift if odd and outward is None else value - drift
                value = (
                    value
                    - east[row, x, cut] * (after[cut] - before[cut])
                    - upward[row, x, cut] * (up - down)
                )
                new[k][x, cut] = value
                values.append(value)
            if not last and k > 0:
                low, high = values[0][0:1], values[-1][TILE - 1 : TILE]
                extra[0][k, pl.ds(x, 1)] = either(even_lev, high, low)
                extra[1][k, pl.ds(x, 1)] = either(even_lev, low, high)
            return jnp.concatenate(values, axis=0)

        start = either(even_lon, far_lon[k], near_lon[k])
        stop = either(even_lon, near_lon[k], far_lon[k])

        def body(x, carry):
            before, here, total = carry
            after = state[k][x + 1]
            value = cell(x, before, here, after)
            return here, after, (total + value if last else total)

        zero = jnp.zeros((levels, members), jnp.float32)
        before, here, total = lax.fori_loop(
            0, length - 1, body, (start, state[k][0], zero), unroll=UNROLL
        )
        value = cell(length - 1, before, here, stop)
        if not last and k > 0:
            low, high = new[k][0], value
            extra[2][k] = either(even_lon, high, low)
            extra[3][k] = either(even_lon, low, high)
        if last and k > 0:
            writes[k - 1].start()
            line_statistics(new[k], total + value, extra[0], 2 * (k - 1))
    if last:
        for write in writes:
            write.wait()


def line_statistics(row, total, out, at):
    length = row.shape[0]
    mean = total * (1.0 / length)

    def body(x, carry):
        away = row[x] - mean
        return carry + away * away

    out[at] = mean
    out[at + 1] = lax.fori_loop(0, length, body, jnp.zeros_like(mean), unroll=4)


def add_halo(offset, place, part, north, halo, out, inner=None):
    rows, sign = roles(place[0])
    size, levels, members = halo.shape

    def body(x, total):
        at = offset + x
        value = part[at] + (RATE + sign * north[rows[0], at]) * halo[x]
        out[x] = value
        if inner is not None:
            inner(at, value)
        return total + value

    zero = jnp.zeros((levels, members), jnp.float32)
    return lax.fori_loop(0, size, body, zero, unroll=4)


def start_row(part, north, halo, out):
    add_halo(0, here(), part, north, halo, out)


def finish_row(last, *refs):
    place = here()
    part, north, halo, done = refs[:4]
    rest = refs[4:]
    size, (levels, members) = done.shape[0], halo.shape[1:]
    if last:
        row, stats = rest
    else:
        old, piece, row, ends = rest[:4], rest[4], rest[5], rest[6:]
        for a, b in zip(old, ends):
            b[1:] = a[1:]
    even_lev, even_lon = place[1] == 0, place[2] == 0

    def send(at, value):
        if not last:
            low, high = value[0:1], value[levels - 1 : levels]
            ends[0][0, pl.ds(at, 1)] = either(even_lev, high, low)
            ends[1][0, pl.ds(at, 1)] = either(even_lev, low, high)

    def keep(x, total):
        value = done[x]
        row[x] = value
        send(x, value)
        return total + value

    def both(at, value):
        if not last:
            row[at] = value
        send(at, value)

    zero = jnp.zeros((levels, members), jnp.float32)
    total = lax.fori_loop(0, size, keep, zero, unroll=4)
    if last:
        total += add_halo(size, place, part, north, halo, row.at[pl.ds(size, halo.shape[0])])
        line_statistics(row, total, stats, 0)
    else:
        add_halo(size, place, part, north, halo, piece, both)
        low, high = row[0], row[row.shape[0] - 1]
        ends[2][0] = either(even_lon, high, low)
        ends[3][0] = either(even_lon, low, high)


def normalise(count, *refs):
    state, stats = refs[:count], refs[count : count + 4]
    rows, _ = roles(here()[0])
    copies = []
    if count == 1:
        out, end, work, sems = refs[-4:]
        copies.append(pltpu.make_async_copy(state[0], end.at[rows[0]], sems.at[0]))
        copies[0].start()
        rows = rows[:1]
    else:
        out, work, sems = refs[-3:]
        rows = rows[1:]
    length = state[0].shape[0]
    half = length // 2
    for k in range(count):
        means = [s[2 * k] for s in stats]
        mean = 0.25 * ((means[0] + means[1]) + (means[2] + means[3]))
        square = (stats[0][2 * k + 1] + stats[1][2 * k + 1]) + (
            stats[2][2 * k + 1] + stats[3][2 * k + 1]
        )
        for part in means:
            square += length * ((part - mean) * (part - mean))
        scale = lax.rsqrt(square * (1.0 / (4 * length)) + 0.0001)

        def body(x, carry):
            work[k, x] = (state[k][x] - mean) * scale
            return carry

        for h in range(2):
            lax.fori_loop(half * h, half * (h + 1), body, 0, unroll=4)
            cut = pl.ds(half * h, half)
            copies.append(
                pltpu.make_async_copy(
                    work.at[k, cut], out.at[rows[k], cut], sems.at[1 + 2 * k + h]
                )
            )
            copies[-1].start()
    for copy in copies:
        copy.wait()


def placed(array, space):
    return pltpu.with_memory_space_constraint(array, space)


def shards(initial_state, north, east, upward):
    rows_here, length, levels, members = initial_state.shape
    row_type = jax.ShapeDtypeStruct((length, levels, members), jnp.float32)
    sizes = (length * FIRST // 96, length - length * FIRST // 96)
    piece_types = [jax.ShapeDtypeStruct((n, levels, members), jnp.float32) for n in sizes]
    lev_type = jax.ShapeDtypeStruct((rows_here, length, members), jnp.float32)
    lon_type = jax.ShapeDtypeStruct((rows_here, levels, members), jnp.float32)
    whole = jax.ShapeDtypeStruct(initial_state.shape, jnp.float32)
    vmem = pl.BlockSpec(memory_space=pltpu.VMEM)
    anywhere = pl.BlockSpec(memory_space=pl.ANY)

    def call(kernel, args, outs, flops, aliases={}, in_specs=None, out_specs=None, scratch=(), room=2**20):
        return pl.pallas_call(
            kernel,
            out_shape=outs,
            in_specs=in_specs or [vmem] * len(args),
            out_specs=out_specs or [vmem] * len(outs),
            scratch_shapes=list(scratch),
            input_output_aliases=aliases,
            compiler_params=pltpu.CompilerParams(vmem_limit_bytes=room),
            cost_estimate=pl.CostEstimate(flops=flops, bytes_accessed=0, transcendentals=0),
        )(*args)

    lats, lons = lax.axis_size("lat"), lax.axis_size("lon")

    def pairs(count, start):
        out = []
        for i in range(start, count - 1, 2):
            out += [(i, i + 1), (i + 1, i)]
        return out

    def across(array):
        return lax.ppermute(array, "lat", pairs(lats, 1))

    def beside(array):
        return lax.ppermute(array, "lat", pairs(lats, 0))

    def swap(array, axis, start):
        return lax.ppermute(array, axis, pairs(lax.axis_size(axis), start))

    def ends_of(near_lev, far_lev, near_lon, far_lon):
        return [
            swap(near_lev, "lev", 0),
            swap(far_lev, "lev", 1),
            swap(near_lon, "lon", 0),
            swap(far_lon, "lon", 1),
        ]

    def from_others(array):
        made = []
        for d in (1, 2, 3):
            made.append(lax.ppermute(array, "lon", [(i, i ^ d) for i in range(lons)]))
        return made

    stats_type = jax.ShapeDtypeStruct((2 * rows_here - 2, levels, members), jnp.float32)
    end_types = [lev_type, lev_type, lon_type, lon_type]
    source = placed(initial_state, pltpu.HBM)
    winds = [placed(north, pltpu.VMEM), placed(east, pltpu.VMEM), placed(upward, pltpu.HBM)]
    for step in range(STEPS):
        last = step == STEPS - 1
        if step == 0:
            pieces = call(
                take_outer,
                [source],
                piece_types,
                10**6,
                in_specs=[anywhere],
                scratch=[pltpu.SemaphoreType.DMA((PIECES,))],
            )
            halos = [across(piece) for piece in pieces]
            outer, *inner_rows, near, far, close, distant = call(
                take_all,
                [source],
                [row_type] * 4 + end_types,
                10**9,
                in_specs=[anywhere],
                scratch=[pltpu.SemaphoreType.DMA((4,))],
            )
            core_row = beside(inner_rows[2])
            ends = ends_of(near, far, close, distant)
        else:
            (begun,) = call(
                start_row, [part, winds[0], halos[0]], piece_types[:1], 10**9
            )
            first_halo = across(begun)
            ended, outer, *sent = call(
                functools.partial(finish_row, False),
                [part, winds[0], halos[1], begun, *extra],
                [piece_types[1], row_type, *end_types],
                10**9,
            )
            halos = [first_halo, across(ended)]
            ends = ends_of(*sent)
        part, *made = call(
            functools.partial(spread_step, step == 0, last),
            [outer, *inner_rows, core_row, *ends, *winds],
            [row_type] * 4
            + ([stats_type, whole] if last else end_types)
            + ([whole] if step == 0 else []),
            SPREAD_FLOPS,
            in_specs=[vmem] * 11 + [anywhere if step == 0 else vmem],
            out_specs=[vmem] * 5 + [anywhere] if last else None,
            scratch=[pltpu.SemaphoreType.DMA((4,))] if step == 0 or last else [],
        )
        if step == 0:
            winds[2] = placed(made.pop(), pltpu.VMEM)
        if last:
            end = made.pop()
        inner_rows, extra = made[:3], made[3:]
        if not last:
            core_row = beside(inner_rows[2])

    def normalised(rows_of, stats, others, *results):
        count = len(rows_of)
        return call(
            functools.partial(normalise, count),
            [*rows_of, stats, *others, *results],
            [whole] * max(1, len(results)),
            10**9,
            aliases={count + 4 + i: i for i in range(len(results))},
            in_specs=[vmem] * (count + 4) + [anywhere] * len(results),
            out_specs=[anywhere] * max(1, len(results)),
            scratch=[
                pltpu.VMEM((count, length, levels, members), jnp.float32),
                pltpu.SemaphoreType.DMA((1 + 2 * count,)),
            ],
            room=8 * 2**20,
        )

    (begun,) = call(start_row, [part, winds[0], halos[0]], piece_types[:1], 10**9)
    early = from_others(extra[0])
    outer, stats = call(
        functools.partial(finish_row, True),
        [part, winds[0], halos[1], begun],
        [row_type, jax.ShapeDtypeStruct((2, levels, members), jnp.float32)],
        10**9,
    )
    late = from_others(stats)
    results = normalised(inner_rows, extra[0], early)
    return tuple(normalised([outer], stats, late, *results, end))


SPREAD_FLOPS = 2 * 10**10


def solution(mesh):
    return jax.shard_map(
        shards, mesh=mesh, in_specs=(GRID,) * 4, out_specs=(GRID, GRID), check_vma=False
    )
```
